32 devices in a mesh: runs: 1, cfg: 32 (over z, y, x, core).
Axes of the slice: x: 2, y: 2, z: 4, core: 2. Of those that a mesh axis runs over, the one named last changes fastest.
Arguments:
- amplitudes: float32 [2, 512, 128, 512], P('runs', 'cfg')
- prop_third: float32 [2, 512, 512], replicated
- bitmasks_first: int32 [512], replicated, may hold values from 0 to 10922, as said below
- bitmasks_second: int32 [128], replicated, may hold values from 0 to 10922, as said below
- bitmasks_third: int32 [512], P('cfg'), may hold values from 0 to 10922, as said below
- detune_steps: int32 [3], P('runs'), may hold values from 0 to 15
Outputs:
- density: float32 [512, 2, 512], P(('runs', 'cfg'))
The draws below stay inside these ranges and needn't reach their ends.
Inputs may be any that keep to these rules, and one draw needn't show every extreme that they name: `bitmasks_first`: 512 different numbers, none with two adjacent bits set. `bitmasks_second`: 128 different numbers, none with two adjacent bits set. `bitmasks_third`: 512 different numbers, none with two adjacent bits set.
All inputs are finite; a program needn't handle non-finite values.
Results may differ from the reference program's by a relative error of at most 0.00005.
Values sent between devices are 32-bit elements; how exact they have to be, the bound alone decides.
No kernel may reach another device: no remote copies, remote signals or barrier semaphores. Data moves between devices by JAX's collectives and lax.ppermute only.
A program may use at most 64 MiB of HBM per device.

```python
import math
import jax
import jax.numpy as jnp
from jax import lax

NA = 512
NB = 128
NC = 512


factor_count = 16


def independent_sets(key, wanted):
    candidates = jnp.arange(16384, dtype=jnp.int32)
    valid = candidates & jnp.right_shift(candidates, 1) == 0
    scores = jax.random.randint(key, (16384,), 0, 16384, dtype=jnp.int32) * 16384 + candidates
    scores = jnp.where(valid, scores, 268435456 + candidates)
    order = jnp.argsort(scores, stable=True)
    return candidates[order[:wanted]]


def propagator(key, width):
    noise = jax.random.normal(key, (2, width, width), jnp.float32)
    noise = noise * (0.6 / math.sqrt(2.0 * width))
    identity = jnp.eye(width, dtype=jnp.float32)
    return noise + jnp.stack([identity, jnp.zeros_like(identity)])


def draw_amplitudes(key, part):
    keys = jax.random.split(jax.random.fold_in(key, 11), 3)
    left = jax.random.normal(keys[0], (2, NC * NB, factor_count), jnp.float32)
    right = jax.random.normal(keys[1], (2, factor_count, NA), jnp.float32)
    noise = jax.random.normal(keys[2], (2, NC * NB, NA), jnp.float32)
    low_real = jnp.dot(left[0], right[0]) - jnp.dot(left[1], right[1])
    low_imag = jnp.dot(left[0], right[1]) + jnp.dot(left[1], right[0])
    low = jnp.stack([low_real, low_imag]) / math.sqrt(2.0 * factor_count)
    full = (low + 0.5 * noise) / math.sqrt(1.0 * NC * NB)
    return full.reshape(2, NC, NB, NA)


def draw_prop_third(key, part):
    return propagator(jax.random.fold_in(key, 23), NC)


def draw_bitmasks_first(key, part):
    return independent_sets(jax.random.fold_in(key, 31), NA)


def draw_bitmasks_second(key, part):
    return independent_sets(jax.random.fold_in(key, 32), NB)


def draw_bitmasks_third(key, part):
    return independent_sets(jax.random.fold_in(key, 33), NC)


def setup_inputs(seed: int = 0, part: int = 0) -> dict:
    splits = jax.random.split(jax.random.key(seed), 7)
    part_keys = jax.random.split(jax.random.fold_in(splits[6], part), 7)
    return {
        "amplitudes": draw_amplitudes(jax.random.fold_in(jax.random.fold_in(splits[6], part), 71), part),
        "prop_third": draw_prop_third(jax.random.fold_in(splits[6], 71), part),
        "bitmasks_first": draw_bitmasks_first(jax.random.fold_in(splits[6], 71), part),
        "bitmasks_second": draw_bitmasks_second(jax.random.fold_in(splits[6], 71), part),
        "bitmasks_third": draw_bitmasks_third(jax.random.fold_in(splits[6], 71), part),
        "detune_steps": jax.random.randint(part_keys[5], (3,), 0, 16).astype(jnp.int32),
    }


angle_step = 0.2
pair_angle = 0.7
atom_count = 14


def atom_bit(bitmasks, which):
    return (jnp.right_shift(bitmasks, which) & 1).astype(jnp.float32)


def occupation(bitmasks):
    total = jnp.zeros(bitmasks.shape, jnp.float32)
    for which in range(atom_count):
        total = total + atom_bit(bitmasks, which)
    return total


def boundary_terms(first, second, third, detune_steps):
    scaled = detune_steps.astype(jnp.float32) * angle_step
    phase_first = scaled[0] * occupation(first)
    phase_second = scaled[1] * occupation(second)
    phase_third = scaled[2] * occupation(third)
    last_first = atom_bit(first, 13)[None, None, :]
    near_first = atom_bit(first, 12)[None, None, :]
    head_second = atom_bit(second, 0)[None, :, None]
    next_second = atom_bit(second, 1)[None, :, None]
    last_second = atom_bit(second, 13)[None, :, None]
    near_second = atom_bit(second, 12)[None, :, None]
    head_third = atom_bit(third, 0)[:, None, None]
    next_third = atom_bit(third, 1)[:, None, None]
    allowed = (1.0 - last_first * head_second) * (1.0 - last_second * head_third)
    pairs = near_first * head_second + last_first * next_second + near_second * head_third + last_second * next_third
    angle = phase_third[:, None, None] + phase_second[None, :, None] + phase_first[None, None, :] + pair_angle * pairs
    return allowed, angle


def apply_third(real_part, imag_part, prop):
    def product(values, matrix):
        return jnp.einsum("ij,jba->iba", matrix, values, precision=lax.Precision.HIGHEST)
    return (product(real_part, prop[0]) - product(imag_part, prop[1]),
            product(real_part, prop[1]) + product(imag_part, prop[0]))


def apply_phases(real_part, imag_part, allowed, angle):
    cosine = jnp.cos(angle)
    sine = jnp.sin(angle)
    return (allowed * (real_part * cosine + imag_part * sine),
            allowed * (imag_part * cosine - real_part * sine))


def inner_rows(left, right):
    return lax.dot_general(left, right, (((0,), (0,)), ((), ())), precision=lax.Precision.HIGHEST,
                           preferred_element_type=jnp.float32)


def reference(amplitudes, prop_third, bitmasks_first, bitmasks_second, bitmasks_third, detune_steps):
    allowed, angle = boundary_terms(bitmasks_first, bitmasks_second, bitmasks_third, detune_steps)
    real_part, imag_part = apply_phases(amplitudes[0], amplitudes[1], allowed, angle)
    real_part, imag_part = apply_third(real_part, imag_part, prop_third)
    width = real_part.shape[2]
    flat_real = real_part.reshape(-1, width)
    flat_imag = imag_part.reshape(-1, width)
    density_real = inner_rows(flat_real, flat_real) + inner_rows(flat_imag, flat_imag)
    density_imag = inner_rows(flat_imag, flat_real) - inner_rows(flat_real, flat_imag)
    return jnp.stack([density_real, density_imag], axis=1)
```

```python
import jax
import jax.numpy as jnp
from jax import lax
from jax.experimental import pallas as pl
from jax.experimental.pallas import tpu as pltpu
from jax.sharding import PartitionSpec as P

angle_step = 0.2
pair_angle = 0.7
atom_count = 14
tile = 128


def bit(masks, which):
    return (jnp.right_shift(masks, which) & 1).astype(jnp.float32)


def occupation(masks):
    total = bit(masks, 0)
    for which in range(1, atom_count):
        total = total + bit(masks, which)
    return total


def high_low(values):
    high = values.astype(jnp.bfloat16)
    low = (values - high.astype(jnp.float32)).astype(jnp.bfloat16)
    return high, low


def pack_body(shape, steps, third, second_smem, first, second, amps, packed, row_re, row_im, col_re, col_im):
    rows, seconds, owned, width = shape

    @pl.when((pl.program_id(0) == 0) & (pl.program_id(1) == 0))
    def tables():
        scale_first = steps[0].astype(jnp.float32) * angle_step
        scale_second = steps[1].astype(jnp.float32) * angle_step
        scale_third = steps[2].astype(jnp.float32) * angle_step
        kind = lax.broadcasted_iota(jnp.int32, (8, width), 0)
        masks = jnp.broadcast_to(first[...], (8, width))
        head = bit(kind, 0)
        angle = scale_first * occupation(masks) + pair_angle * (
            bit(masks, 12) * head + bit(masks, 13) * bit(kind, 1)
        )
        allowed = 1.0 - bit(masks, 13) * head
        table_re = allowed * jnp.cos(angle)
        table_im = -allowed * jnp.sin(angle)
        for index in range(width // tile):
            row_re[pl.ds(8 * index, 8), :] = table_re[:, index * tile : (index + 1) * tile]
            row_im[pl.ds(8 * index, 8), :] = table_im[:, index * tile : (index + 1) * tile]
        place = lax.broadcasted_iota(jnp.int32, (rows, seconds), 0)
        masks_third = jnp.zeros((rows, seconds), jnp.int32)
        for row in range(rows):
            masks_third = jnp.where(place == row, third[row], masks_third)
        masks_second = jnp.broadcast_to(second[...], (rows, seconds))
        last = bit(masks_second, 13)
        angle = (
            scale_third * occupation(masks_third)
            + scale_second * occupation(masks_second)
            + pair_angle * (bit(masks_second, 12) * bit(masks_third, 0) + last * bit(masks_third, 1))
        )
        allowed = 1.0 - last * bit(masks_third, 0)
        col_re[...] = allowed * jnp.cos(angle)
        col_im[...] = -allowed * jnp.sin(angle)

    here = pl.ds(pl.multiple_of(pl.program_id(0) * 8, 8), 8)
    base = pl.program_id(1) * 8
    columns_re = col_re[here, :]
    columns_im = col_im[here, :]
    for second_state in range(seconds):
        kind = base + (second_smem[second_state] & 3)
        across_re = row_re[pl.ds(kind, 1), :]
        across_im = row_im[pl.ds(kind, 1), :]
        down_re = columns_re[:, second_state : second_state + 1]
        down_im = columns_im[:, second_state : second_state + 1]
        turn_re = down_re * across_re - down_im * across_im
        turn_im = down_re * across_im + down_im * across_re
        real = amps[0, pl.ds(second_state, 8, stride=seconds), :]
        imag = amps[1, pl.ds(second_state, 8, stride=seconds), :]
        target, slot = second_state // owned, second_state % owned
        lanes = pl.ds(slot * tile, tile)
        packed[target, 0, :, lanes] = real * turn_re - imag * turn_im
        packed[target, 1, :, lanes] = real * turn_im + imag * turn_re


def pack(amps, first, second, third, steps, devices):
    _, rows, seconds, width = amps.shape
    owned = seconds // devices
    smem = pl.BlockSpec(memory_space=pltpu.SMEM)
    whole = lambda n: pl.BlockSpec((1, n), lambda i, j: (0, 0))
    return pl.pallas_call(
        lambda *refs: pack_body((rows, seconds, owned, width), *refs),
        grid=(rows // 8, width // tile),
        in_specs=[smem, smem, smem, whole(width), whole(seconds),
                  pl.BlockSpec((2, 8 * seconds, tile), lambda i, j: (0, i, j))],
        out_specs=pl.BlockSpec((devices, 2, 8, owned * tile), lambda i, j: (0, 0, i, j)),
        out_shape=jax.ShapeDtypeStruct((devices, 2, rows, owned * width), jnp.float32),
        scratch_shapes=[pltpu.VMEM((8 * width // tile, tile), jnp.float32)] * 2 + [pltpu.VMEM((rows, seconds), jnp.float32)] * 2,
        compiler_params=pltpu.CompilerParams(dimension_semantics=("arbitrary", "arbitrary")),
        name="pack",
    )(steps, third, second, first.reshape(1, -1), second.reshape(1, -1), amps.reshape(2, rows * seconds, width))


def density_body(parity_axis, tiles, prop, *refs):
    parts = refs[:tiles]
    keep, send, matrix, values, evolved, square, cross = refs[tiles:]
    step = pl.program_id(0)
    n = prop.shape[1]
    width = tiles * tile

    @pl.when(step == 0)
    def prepare():
        for plane, sign, row, column in ((0, 1, 0, 0), (1, -1, 0, 1), (1, 1, 1, 0), (0, 1, 1, 1)):
            high, low = high_low(prop[plane])
            if sign < 0:
                high, low = -high, -low
            rows = pl.ds(row * n, n)
            matrix[rows, pl.ds(column * n, n)] = high
            matrix[rows, pl.ds((2 + column) * n, n)] = high
            matrix[rows, pl.ds((4 + column) * n, n)] = low
        square[...] = jnp.zeros_like(square)
        cross[...] = jnp.zeros_like(cross)

    for plane in range(2):
        for index, part in enumerate(parts):
            high, low = high_low(part[:, plane].reshape(n, tile))
            lanes = pl.ds(index * tile, tile)
            values[pl.ds(plane * n, n), lanes] = high
            values[pl.ds((2 + plane) * n, n), lanes] = low
            values[pl.ds((4 + plane) * n, n), lanes] = high

    block = 256

    def evolve(index, carry):
        rows = pl.ds(pl.multiple_of(index * block, block), block)
        evolved[rows, :] = jnp.dot(matrix[rows, :], values[...], preferred_element_type=jnp.float32)
        return carry

    lax.fori_loop(0, 2 * n // block, evolve, 0)

    high, low = high_low(evolved[...])
    both = jnp.concatenate([high, low], axis=1)
    turned_high = high.T
    turned_low = low[n:].T
    square[...] += jnp.dot(turned_high, both, preferred_element_type=jnp.float32)
    cross[...] += (
        jnp.dot(turned_high[:, n:], high[:n], preferred_element_type=jnp.float32)
        + jnp.dot(turned_high[:, n:], low[:n], preferred_element_type=jnp.float32)
        + jnp.dot(turned_low, high[:n], preferred_element_type=jnp.float32)
    )

    @pl.when(step == pl.num_programs(0) - 1)
    def finish():
        mixed = square[:, width:]
        square[:, :width] = square[:, :width] + mixed + mixed.T
        square[:, width:] = cross[...] - cross[...].T
        parity = lax.rem(lax.axis_index(parity_axis), 2)
        own = keep.shape[1]
        for chip in range(keep.shape[0]):
            near = pl.multiple_of((2 * chip + parity) * own, own)
            far = pl.multiple_of((2 * chip + 1 - parity) * own, own)
            keep[chip] = square[pl.ds(near, own), :]
            send[chip] = square[pl.ds(far, own), :]


def density(prop, parts, width, devices):
    n = prop.shape[1]
    sources, _, rows, lanes = parts.shape
    own = width // devices
    tiles, slots = width // tile, lanes // width
    half = jax.ShapeDtypeStruct((devices // 2, own, 2 * width), jnp.float32)
    fixed = pl.BlockSpec((devices // 2, own, 2 * width), lambda i: (0, 0, 0))
    return pl.pallas_call(
        lambda *refs: density_body("cfg", tiles, *refs),
        grid=(slots,),
        in_specs=[pl.BlockSpec((2, n, n), lambda i: (0, 0, 0)),
                  *(pl.BlockSpec((sources, 2, rows, tile), lambda i, t=t: (0, 0, 0, t * slots + i)) for t in range(tiles))],
        out_specs=(fixed, fixed),
        out_shape=(half, half),
        scratch_shapes=[
            pltpu.VMEM((2 * n, 6 * n), jnp.bfloat16),
            pltpu.VMEM((6 * n, width), jnp.bfloat16),
            pltpu.VMEM((2 * n, width), jnp.float32),
            pltpu.VMEM((width, 2 * width), jnp.float32),
            pltpu.VMEM((width, width), jnp.float32),
        ],
        compiler_params=pltpu.CompilerParams(dimension_semantics=("arbitrary",), vmem_limit_bytes=60 * 2**20),
        name="density",
    )(prop, *[parts] * tiles)


def shards(amplitudes, prop_third, first, second, third, steps, devices):
    width = amplitudes.shape[3]
    packed = pack(amplitudes, first, second, third, steps, devices)
    parts = lax.all_to_all(packed, "cfg", split_axis=0, concat_axis=0, tiled=True)
    keep, send = density(prop_third, parts, width, devices)
    swap = [(i, i ^ 1) for i in range(devices)]
    half = keep + lax.ppermute(send, "cfg", swap)
    groups = [list(range(core, devices, 2)) for core in range(2)]
    pieces = lax.all_to_all(half, "cfg", split_axis=0, concat_axis=0, tiled=True, axis_index_groups=groups)
    return jnp.sum(pieces, axis=0).reshape(-1, 2, width)


def boundary_terms(first, second, third, detune_steps):
    scaled = detune_steps.astype(jnp.float32) * angle_step
    phase_first = scaled[0] * occupation(first)
    phase_second = scaled[1] * occupation(second)
    phase_third = scaled[2] * occupation(third)
    last_first = bit(first, 13)[None, None, :]
    near_first = bit(first, 12)[None, None, :]
    head_second = bit(second, 0)[None, :, None]
    next_second = bit(second, 1)[None, :, None]
    last_second = bit(second, 13)[None, :, None]
    near_second = bit(second, 12)[None, :, None]
    head_third = bit(third, 0)[:, None, None]
    next_third = bit(third, 1)[:, None, None]
    allowed = (1.0 - last_first * head_second) * (1.0 - last_second * head_third)
    pairs = (
        near_first * head_second
        + last_first * next_second
        + near_second * head_third
        + last_second * next_third
    )
    angle = (
        phase_third[:, None, None]
        + phase_second[None, :, None]
        + phase_first[None, None, :]
        + pair_angle * pairs
    )
    return (allowed, angle)


def apply_third(block, prop):

    def product(values, matrix):
        return jnp.einsum("ij,jba->iba", matrix, values, precision=lax.Precision.HIGHEST)

    real_part = product(block[0], prop[0]) - product(block[1], prop[1])
    imag_part = product(block[0], prop[1]) + product(block[1], prop[0])
    return jnp.stack([real_part, imag_part])


def inner_rows(left, right):
    return lax.dot_general(
        left,
        right,
        (((0,), (0,)), ((), ())),
        precision=lax.Precision.HIGHEST,
        preferred_element_type=jnp.float32,
    )


def plain_shards(amplitudes, prop_third, bitmasks_first, bitmasks_second, bitmasks_third, detune_steps):
    allowed, angle = boundary_terms(bitmasks_first, bitmasks_second, bitmasks_third, detune_steps)
    cosine = jnp.cos(angle)
    sine = jnp.sin(angle)
    phased = jnp.stack(
        [
            allowed * (amplitudes[0] * cosine + amplitudes[1] * sine),
            allowed * (amplitudes[1] * cosine - amplitudes[0] * sine),
        ]
    )
    evolved = apply_third(
        lax.all_to_all(phased, "cfg", split_axis=2, concat_axis=1, tiled=True), prop_third
    )
    width = evolved.shape[3]
    flat_real = evolved[0].reshape(-1, width)
    flat_imag = evolved[1].reshape(-1, width)
    stacked = jnp.concatenate([flat_real, flat_imag], axis=0)
    local_real = inner_rows(stacked, stacked)
    crossed = inner_rows(flat_imag, flat_real)
    local_term = jnp.stack([local_real, crossed - crossed.T], axis=1)
    return lax.psum_scatter(local_term, "cfg", scatter_dimension=0, tiled=True)


def solution(mesh):
    devices = mesh.shape["cfg"]

    def body(amplitudes, *others):
        rows = amplitudes.shape[1]
        if rows % 8 or amplitudes.shape[2] % devices or (amplitudes.shape[3] // devices) % 8 or amplitudes.shape[3] % tile:
            return plain_shards(amplitudes, *others)
        return shards(amplitudes, *others, devices)

    placed = (P("runs", "cfg", None, None), P(), P(), P(), P("cfg"), P("runs"))
    return jax.shard_map(
        body,
        mesh=mesh,
        in_specs=placed,
        out_specs=P(("runs", "cfg"), None, None),
        check_vma=False,
    )
```

```python
import jax
import jax.numpy as jnp
from jax import lax
from jax.experimental import pallas as pl
from jax.experimental.pallas import tpu as pltpu
from jax.sharding import PartitionSpec as P

angle_step = 0.2
pair_angle = 0.7
atom_count = 14
tile = 128


def bit(masks, which):
    return (jnp.right_shift(masks, which) & 1).astype(jnp.float32)


def occupation(masks):
    total = bit(masks, 0)
    for which in range(1, atom_count):
        total = total + bit(masks, which)
    return total


def high_low(values):
    high = values.astype(jnp.bfloat16)
    low = (values - high.astype(jnp.float32)).astype(jnp.bfloat16)
    return high, low


def swapped_lanes(values, distance):
    lanes = values.shape[1]
    place = lax.broadcasted_iota(jnp.int32, values.shape, 1)
    up = pltpu.roll(values, lanes - distance, 1)
    down = pltpu.roll(values, distance, 1)
    return jnp.where((place & distance) == 0, up, down)


def pack_body(shape, first_slot, group, place_smem, steps, third, second_smem, first, second, *refs):
    rows, seconds, owned, width, devices, members, slots = shape
    mixed = group is not None
    tiles = width // tile
    amps = [ref.reshape(2, rows * members * owned, tile) for ref in refs[:tiles]]
    row_re, row_im, col_re, col_im = refs[-4:]
    packed = refs[tiles:-4]
    me = place_smem[0] & (members - 1) if mixed else 0
    offset = place_smem[1] * (members * owned) if mixed else 0

    def tables():
        scale_first = steps[0].astype(jnp.float32) * angle_step
        scale_second = steps[1].astype(jnp.float32) * angle_step
        scale_third = steps[2].astype(jnp.float32) * angle_step
        kind = lax.broadcasted_iota(jnp.int32, (8, width), 0)
        masks = jnp.broadcast_to(first[...], (8, width))
        head = bit(kind, 0)
        angle = scale_first * occupation(masks) + pair_angle * (
            bit(masks, 12) * head + bit(masks, 13) * bit(kind, 1)
        )
        allowed = 1.0 - bit(masks, 13) * head
        table_re = allowed * jnp.cos(angle)
        table_im = -allowed * jnp.sin(angle)
        for index in range(tiles):
            row_re[pl.ds(8 * index, 8), :] = table_re[:, index * tile : (index + 1) * tile]
            row_im[pl.ds(8 * index, 8), :] = table_im[:, index * tile : (index + 1) * tile]
        place = lax.broadcasted_iota(jnp.int32, (rows, seconds), 0)
        masks_third = jnp.zeros((rows, seconds), jnp.int32)
        for row in range(rows):
            masks_third = jnp.where(place == row, third[row], masks_third)
        masks_second = jnp.broadcast_to(second[...], (rows, seconds))
        if mixed:
            distance, change = 1, place_smem[2]
            while distance < devices:
                masks_second = jnp.where(
                    (change & distance) != 0, swapped_lanes(masks_second, distance * owned), masks_second
                )
                distance *= 2
        last = bit(masks_second, 13)
        angle = (
            scale_third * occupation(masks_third)
            + scale_second * occupation(masks_second)
            + pair_angle * (bit(masks_second, 12) * bit(masks_third, 0) + last * bit(masks_third, 1))
        )
        allowed = 1.0 - last * bit(masks_third, 0)
        col_re[...] = allowed * jnp.cos(angle)
        col_im[...] = -allowed * jnp.sin(angle)

    tables()
    stride = members * owned
    for target in range(members):
        for slot in range(first_slot, first_slot + slots):
            state = (me ^ target) * owned + slot
            kind = second_smem[offset + state] & 3
            column = target * owned + slot
            out = packed[target] if mixed else packed[0].at[target]
            for half in range(0, rows, 8):
                down_re = col_re[pl.ds(half, 8), column : column + 1]
                down_im = col_im[pl.ds(half, 8), column : column + 1]
                for index in range(tiles):
                    across_re = row_re[pl.ds(8 * index + kind, 1), :]
                    across_im = row_im[pl.ds(8 * index + kind, 1), :]
                    turn_re = down_re * across_re - down_im * across_im
                    turn_im = down_re * across_im + down_im * across_re
                    real = amps[index][0, pl.ds(half * stride + state, 8, stride=stride), :]
                    imag = amps[index][1, pl.ds(half * stride + state, 8, stride=stride), :]
                    lanes = pl.ds((slot - first_slot) * width + index * tile, tile)
                    out[0, pl.ds(half, 8), lanes] = real * turn_re - imag * turn_im
                    out[1, pl.ds(half, 8), lanes] = real * turn_im + imag * turn_re


def pack(amps, first, second, third, steps, devices, first_slot, slots, group, members):
    _, rows, seconds, width = amps.shape
    tiles = width // tile
    owned = seconds // devices
    smem = pl.BlockSpec(memory_space=pltpu.SMEM)
    whole = lambda n: pl.BlockSpec((1, n), lambda i, at: (0, 0))
    if group is not None:
        out_specs = tuple(pl.BlockSpec((2, rows, slots * width), lambda i, at: (0, 0, 0)) for _ in range(members))
        out_shape = tuple(jax.ShapeDtypeStruct((2, rows, slots * width), jnp.float32) for _ in range(members))
        me = lax.axis_index("cfg")
        plane = jnp.right_shift(me, members.bit_length() - 1) ^ group
        place = jnp.stack([me, plane, me ^ (group * members)])
    else:
        members = devices
        out_specs = pl.BlockSpec((devices, 2, rows, slots * width), lambda i, at: (0, 0, 0, 0))
        out_shape = jax.ShapeDtypeStruct((devices, 2, rows, slots * width), jnp.float32)
        place = jnp.zeros((3,), jnp.int32)
    shape = (rows, seconds, owned, width, devices, members, slots)
    return pl.pallas_call(
        lambda *refs: pack_body(shape, first_slot, group, *refs),
        grid_spec=pltpu.PrefetchScalarGridSpec(
            num_scalar_prefetch=1,
            grid=(1,),
            in_specs=[smem, smem, smem, whole(width), whole(seconds),
                      *(pl.BlockSpec((2, rows, members * owned, tile), lambda i, at, t=t: (0, 0, at[1], t)) for t in range(tiles))],
            out_specs=out_specs,
            scratch_shapes=[pltpu.VMEM((8 * tiles, tile), jnp.float32)] * 2 + [pltpu.VMEM((rows, seconds), jnp.float32)] * 2,
        ),
        out_shape=out_shape,
        compiler_params=pltpu.CompilerParams(dimension_semantics=("arbitrary",)),
        cost_estimate=pl.CostEstimate(flops=24 * amps.size, bytes_accessed=8 * amps.size, transcendentals=0),
    )(place, steps, third, second, first.reshape(1, -1), second.reshape(1, -1), *[amps] * tiles)


def spread_propagator(prop, matrix):
    n = prop.shape[1]
    for plane, sign, row, column in ((0, 1, 0, 0), (1, -1, 0, 1), (1, 1, 1, 0), (0, 1, 1, 1)):
        high, low = high_low(prop[plane])
        if sign < 0:
            high, low = -high, -low
        rows = pl.ds(row * n, n)
        matrix[rows, pl.ds(column * n, n)] = high
        matrix[rows, pl.ds((2 + column) * n, n)] = low


def add_block(matrix, values, evolved, sums, ready=None):
    n = matrix.shape[0] // 2
    width = sums.shape[0]
    square, cross = sums.at[:, pl.ds(0, 2 * width)], sums.at[:, pl.ds(2 * width, width)]
    block = 256

    def evolve(index, carry):
        rows = pl.ds(pl.multiple_of(index * block, block), block)
        high = matrix[rows, pl.ds(0, 2 * n)]
        low = matrix[rows, pl.ds(2 * n, 2 * n)]
        evolved[rows, :] = (
            jnp.dot(high, values[pl.ds(0, 2 * n), :], preferred_element_type=jnp.float32)
            + jnp.dot(high, values[pl.ds(2 * n, 2 * n), :], preferred_element_type=jnp.float32)
            + jnp.dot(low, values[pl.ds(0, 2 * n), :], preferred_element_type=jnp.float32)
        )
        return carry

    lax.fori_loop(0, 2 * n // block, evolve, 0)
    if ready is not None:
        ready()
    high, low = high_low(evolved[...])
    both = jnp.concatenate([high, low], axis=1)
    turned_high = high.T
    turned_low = low[n:].T
    square[...] += jnp.dot(turned_high, both, preferred_element_type=jnp.float32)
    cross[...] += (
        jnp.dot(turned_high[:, n:], high[:n], preferred_element_type=jnp.float32)
        + jnp.dot(turned_high[:, n:], low[:n], preferred_element_type=jnp.float32)
        + jnp.dot(turned_low, high[:n], preferred_element_type=jnp.float32)
    )


def fill(values, n, plane, start, rows, block):
    high, low = high_low(block)
    values[pl.ds(plane * n + start, rows), :] = high
    values[pl.ds((2 + plane) * n + start, rows), :] = low


def density_early_body(count, prop, *refs):
    parts, (sums, matrix, values, evolved) = refs[:count], refs[count:]
    n = prop.shape[1]

    @pl.when(pl.program_id(0) == 0)
    def prepare():
        spread_propagator(prop, matrix)
        sums[...] = jnp.zeros_like(sums)

    me = lax.axis_index("cfg")
    for plane in range(2):
        for index, part in enumerate(parts):
            rows = part.shape[1]
            fill(values, n, plane, pl.multiple_of((me ^ index) * rows, rows), rows, part[plane])
    add_block(matrix, values, evolved, sums)


def density_late_body(matrix_far, parts, sums_far, keep, send, matrix, values, evolved, sums, sems):
    n = matrix.shape[0] // 2
    width = sums.shape[0]
    copies = [
        pltpu.make_async_copy(matrix_far, matrix, sems.at[0]),
        pltpu.make_async_copy(sums_far, sums, sems.at[1]),
    ]
    for copy in copies:
        copy.start()
    for plane in range(2):
        fill(values, n, plane, 0, n, parts[:, plane].reshape(n, width))
    copies[0].wait()

    add_block(matrix, values, evolved, sums, copies[1].wait)
    mixed = sums[:, width : 2 * width]
    cross = sums[:, 2 * width :]
    sums[:, :width] = sums[:, :width] + mixed + mixed.T
    sums[:, width : 2 * width] = cross - cross.T
    parity = lax.rem(lax.axis_index("cfg"), 2)
    own = keep.shape[1]
    for chip in range(keep.shape[0]):
        near = pl.multiple_of((2 * chip + parity) * own, own)
        far = pl.multiple_of((2 * chip + 1 - parity) * own, own)
        keep[chip] = sums[pl.ds(near, own), pl.ds(0, 2 * width)]
        send[chip] = sums[pl.ds(far, own), pl.ds(0, 2 * width)]


def cost(slots, width, n):
    return pl.CostEstimate(flops=slots * width * n * (24 * n + 14 * width), bytes_accessed=2**24, transcendentals=0)


vmem = pl.BlockSpec(memory_space=pltpu.VMEM)
far = pl.BlockSpec(memory_space=pltpu.HBM)


def density_early(prop, parts, width):
    n = prop.shape[1]
    slots = parts[0].shape[-1] // width
    return pl.pallas_call(
        lambda *refs: density_early_body(len(parts), *refs),
        grid=(slots,),
        in_specs=[pl.BlockSpec((2, n, n), lambda i: (0, 0, 0)),
                  *(pl.BlockSpec((2, part.shape[1], width), lambda i: (0, 0, i)) for part in parts)],
        out_specs=(
            pl.BlockSpec((width, 3 * width), lambda i: (0, 0)),
            pl.BlockSpec((2 * n, 4 * n), lambda i: (0, 0)),
        ),
        out_shape=(
            jax.ShapeDtypeStruct((width, 3 * width), jnp.float32),
            jax.ShapeDtypeStruct((2 * n, 4 * n), jnp.bfloat16),
        ),
        scratch_shapes=[
            pltpu.VMEM((4 * n, width), jnp.bfloat16),
            pltpu.VMEM((2 * n, width), jnp.float32),
        ],
        compiler_params=pltpu.CompilerParams(dimension_semantics=("arbitrary",)),
        cost_estimate=cost(slots, width, n),
        name="density_early",
    )(prop, *parts)


def density_late(matrix, parts, sums, devices):
    n = matrix.shape[0] // 2
    width = sums.shape[0]
    half = jax.ShapeDtypeStruct((devices // 2, width // devices, 2 * width), jnp.float32)
    return pl.pallas_call(
        density_late_body,
        in_specs=[far, vmem, far],
        out_specs=(vmem, vmem),
        out_shape=(half, half),
        scratch_shapes=[
            pltpu.VMEM(matrix.shape, jnp.bfloat16),
            pltpu.VMEM((4 * n, width), jnp.bfloat16),
            pltpu.VMEM((2 * n, width), jnp.float32),
            pltpu.VMEM((width, 3 * width), jnp.float32),
            pltpu.SemaphoreType.DMA((2,)),
        ],
        compiler_params=pltpu.CompilerParams(vmem_limit_bytes=48 * 2**20),
        cost_estimate=cost(1, width, n),
        name="density_late",
    )(matrix, parts, sums)


def exchange_order(devices):
    half = devices // 2
    return list(range(half, devices)) + list(range(1, half))


def shards(amplitudes, prop_third, first, second, third, steps, devices):
    width = amplitudes.shape[3]
    owned = amplitudes.shape[2] // devices
    late = 1
    members = devices // 4
    arrived = [None] * devices
    blocks = []
    for group in range(4):
        blocks += pack(amplitudes, first, second, third, steps, devices, 0, owned - late, group, members)
    arrived[0] = blocks[0]
    for distance in exchange_order(devices):
        pairs = [(i, i ^ distance) for i in range(devices)]
        arrived[distance] = lax.ppermute(blocks[distance], "cfg", pairs)
    packed = pack(amplitudes, first, second, third, steps, devices, owned - late, late, None, None)
    parts = lax.all_to_all(packed, "cfg", split_axis=0, concat_axis=0, tiled=True)
    sums, matrix = density_early(prop_third, arrived, width)
    keep, send = density_late(matrix, parts, sums, devices)
    swap = [(i, i ^ 1) for i in range(devices)]
    half = keep + lax.ppermute(send, "cfg", swap)
    groups = [list(range(core, devices, 2)) for core in range(2)]
    pieces = lax.all_to_all(half, "cfg", split_axis=0, concat_axis=0, tiled=True, axis_index_groups=groups)
    return jnp.sum(pieces, axis=0).reshape(-1, 2, width)


def boundary_terms(first, second, third, detune_steps):
    scaled = detune_steps.astype(jnp.float32) * angle_step
    phase_first = scaled[0] * occupation(first)
    phase_second = scaled[1] * occupation(second)
    phase_third = scaled[2] * occupation(third)
    last_first = bit(first, 13)[None, None, :]
    near_first = bit(first, 12)[None, None, :]
    head_second = bit(second, 0)[None, :, None]
    next_second = bit(second, 1)[None, :, None]
    last_second = bit(second, 13)[None, :, None]
    near_second = bit(second, 12)[None, :, None]
    head_third = bit(third, 0)[:, None, None]
    next_third = bit(third, 1)[:, None, None]
    allowed = (1.0 - last_first * head_second) * (1.0 - last_second * head_third)
    pairs = (
        near_first * head_second
        + last_first * next_second
        + near_second * head_third
        + last_second * next_third
    )
    angle = (
        phase_third[:, None, None]
        + phase_second[None, :, None]
        + phase_first[None, None, :]
        + pair_angle * pairs
    )
    return (allowed, angle)


def apply_third(block, prop):

    def product(values, matrix):
        return jnp.einsum("ij,jba->iba", matrix, values, precision=lax.Precision.HIGHEST)

    real_part = product(block[0], prop[0]) - product(block[1], prop[1])
    imag_part = product(block[0], prop[1]) + product(block[1], prop[0])
    return jnp.stack([real_part, imag_part])


def inner_rows(left, right):
    return lax.dot_general(
        left,
        right,
        (((0,), (0,)), ((), ())),
        precision=lax.Precision.HIGHEST,
        preferred_element_type=jnp.float32,
    )


def plain_shards(amplitudes, prop_third, bitmasks_first, bitmasks_second, bitmasks_third, detune_steps):
    allowed, angle = boundary_terms(bitmasks_first, bitmasks_second, bitmasks_third, detune_steps)
    cosine = jnp.cos(angle)
    sine = jnp.sin(angle)
    phased = jnp.stack(
        [
            allowed * (amplitudes[0] * cosine + amplitudes[1] * sine),
            allowed * (amplitudes[1] * cosine - amplitudes[0] * sine),
        ]
    )
    evolved = apply_third(
        lax.all_to_all(phased, "cfg", split_axis=2, concat_axis=1, tiled=True), prop_third
    )
    width = evolved.shape[3]
    flat_real = evolved[0].reshape(-1, width)
    flat_imag = evolved[1].reshape(-1, width)
    stacked = jnp.concatenate([flat_real, flat_imag], axis=0)
    local_real = inner_rows(stacked, stacked)
    crossed = inner_rows(flat_imag, flat_real)
    local_term = jnp.stack([local_real, crossed - crossed.T], axis=1)
    return lax.psum_scatter(local_term, "cfg", scatter_dimension=0, tiled=True)


def solution(mesh):
    devices = mesh.shape["cfg"]

    def body(amplitudes, *others):
        rows = amplitudes.shape[1]
        seconds, width = amplitudes.shape[2:]
        powers = devices & (devices - 1) == 0
        if rows % 16 or seconds != tile or seconds // devices < 2 or (width // devices) % 8 or width % tile or not powers:
            return plain_shards(amplitudes, *others)
        return shards(amplitudes, *others, devices)

    placed = (P("runs", "cfg", None, None), P(), P(), P(), P("cfg"), P("runs"))
    return jax.shard_map(
        body,
        mesh=mesh,
        in_specs=placed,
        out_specs=P(("runs", "cfg"), None, None),
        check_vma=False,
    )
```

```python
import jax
import jax.numpy as jnp
from jax import lax
from jax.experimental import pallas as pl
from jax.experimental.pallas import tpu as pltpu
from jax.sharding import PartitionSpec as P

angle_step = 0.2
pair_angle = 0.7
atom_count = 14
tile = 128


def bit(masks, which):
    return (jnp.right_shift(masks, which) & 1).astype(jnp.float32)


def occupation(masks):
    total = bit(masks, 0)
    for which in range(1, atom_count):
        total = total + bit(masks, which)
    return total


def high_low(values):
    high = values.astype(jnp.bfloat16)
    low = (values - high.astype(jnp.float32)).astype(jnp.bfloat16)
    return high, low


def swapped_lanes(values, distance):
    lanes = values.shape[1]
    place = lax.broadcasted_iota(jnp.int32, values.shape, 1)
    up = pltpu.roll(values, lanes - distance, 1)
    down = pltpu.roll(values, distance, 1)
    return jnp.where((place & distance) == 0, up, down)


def pack_body(shape, first_slot, group, place_smem, steps, third, second_smem, first, second, *refs):
    rows, seconds, owned, width, devices, members, slots = shape
    mixed = group is not None
    tiles = width // tile
    amps = [ref.reshape(2, rows * members * owned, tile) for ref in refs[:tiles]]
    row_re, row_im, col_re, col_im = refs[-4:]
    packed = refs[tiles:-4]
    me = place_smem[0] & (members - 1) if mixed else 0
    offset = place_smem[1] * (members * owned) if mixed else 0

    def tables():
        scale_first = steps[0].astype(jnp.float32) * angle_step
        scale_second = steps[1].astype(jnp.float32) * angle_step
        scale_third = steps[2].astype(jnp.float32) * angle_step
        kind = lax.broadcasted_iota(jnp.int32, (8, width), 0)
        masks = jnp.broadcast_to(first[...], (8, width))
        head = bit(kind, 0)
        angle = scale_first * occupation(masks) + pair_angle * (
            bit(masks, 12) * head + bit(masks, 13) * bit(kind, 1)
        )
        allowed = 1.0 - bit(masks, 13) * head
        table_re = allowed * jnp.cos(angle)
        table_im = -allowed * jnp.sin(angle)
        for index in range(tiles):
            row_re[pl.ds(8 * index, 8), :] = table_re[:, index * tile : (index + 1) * tile]
            row_im[pl.ds(8 * index, 8), :] = table_im[:, index * tile : (index + 1) * tile]
        place = lax.broadcasted_iota(jnp.int32, (rows, seconds), 0)
        masks_third = jnp.zeros((rows, seconds), jnp.int32)
        for row in range(rows):
            masks_third = jnp.where(place == row, third[row], masks_third)
        masks_second = jnp.broadcast_to(second[...], (rows, seconds))
        if mixed:
            distance, change = 1, place_smem[2]
            while distance < devices:
                masks_second = jnp.where(
                    (change & distance) != 0, swapped_lanes(masks_second, distance * owned), masks_second
                )
                distance *= 2
        last = bit(masks_second, 13)
        angle = (
            scale_third * occupation(masks_third)
            + scale_second * occupation(masks_second)
            + pair_angle * (bit(masks_second, 12) * bit(masks_third, 0) + last * bit(masks_third, 1))
        )
        allowed = 1.0 - last * bit(masks_third, 0)
        col_re[...] = allowed * jnp.cos(angle)
        col_im[...] = -allowed * jnp.sin(angle)

    tables()
    stride = members * owned
    for target in range(members):
        for slot in range(first_slot, first_slot + slots):
            state = (me ^ target) * owned + slot
            kind = second_smem[offset + state] & 3
            column = target * owned + slot
            out = packed[target] if mixed else packed[0].at[target]
            for half in range(0, rows, 8):
                down_re = col_re[pl.ds(half, 8), column : column + 1]
                down_im = col_im[pl.ds(half, 8), column : column + 1]
                for index in range(tiles):
                    across_re = row_re[pl.ds(8 * index + kind, 1), :]
                    across_im = row_im[pl.ds(8 * index + kind, 1), :]
                    turn_re = down_re * across_re - down_im * across_im
                    turn_im = down_re * across_im + down_im * across_re
                    real = amps[index][0, pl.ds(half * stride + state, 8, stride=stride), :]
                    imag = amps[index][1, pl.ds(half * stride + state, 8, stride=stride), :]
                    lanes = pl.ds((slot - first_slot) * width + index * tile, tile)
                    out[0, pl.ds(half, 8), lanes] = real * turn_re - imag * turn_im
                    out[1, pl.ds(half, 8), lanes] = real * turn_im + imag * turn_re


def pack(amps, first, second, third, steps, devices, first_slot, slots, group, members):
    _, rows, seconds, width = amps.shape
    tiles = width // tile
    owned = seconds // devices
    smem = pl.BlockSpec(memory_space=pltpu.SMEM)
    whole = lambda n: pl.BlockSpec((1, n), lambda i, at: (0, 0))
    if group is not None:
        out_specs = tuple(pl.BlockSpec((2, rows, slots * width), lambda i, at: (0, 0, 0)) for _ in range(members))
        out_shape = tuple(jax.ShapeDtypeStruct((2, rows, slots * width), jnp.float32) for _ in range(members))
        me = lax.axis_index("cfg")
        plane = jnp.right_shift(me, members.bit_length() - 1) ^ group
        place = jnp.stack([me, plane, me ^ (group * members)])
    else:
        members = devices
        out_specs = pl.BlockSpec((devices, 2, rows, slots * width), lambda i, at: (0, 0, 0, 0))
        out_shape = jax.ShapeDtypeStruct((devices, 2, rows, slots * width), jnp.float32)
        place = jnp.zeros((3,), jnp.int32)
    shape = (rows, seconds, owned, width, devices, members, slots)
    return pl.pallas_call(
        lambda *refs: pack_body(shape, first_slot, group, *refs),
        grid_spec=pltpu.PrefetchScalarGridSpec(
            num_scalar_prefetch=1,
            grid=(1,),
            in_specs=[smem, smem, smem, whole(width), whole(seconds),
                      *(pl.BlockSpec((2, rows, members * owned, tile), lambda i, at, t=t: (0, 0, at[1], t)) for t in range(tiles))],
            out_specs=out_specs,
            scratch_shapes=[pltpu.VMEM((8 * tiles, tile), jnp.float32)] * 2 + [pltpu.VMEM((rows, seconds), jnp.float32)] * 2,
        ),
        out_shape=out_shape,
        compiler_params=pltpu.CompilerParams(dimension_semantics=("arbitrary",)),
        cost_estimate=pl.CostEstimate(flops=24 * amps.size, bytes_accessed=8 * amps.size, transcendentals=0),
    )(place, steps, third, second, first.reshape(1, -1), second.reshape(1, -1), *[amps] * tiles)


def spread_propagator(prop, matrix):
    n = prop.shape[1]
    for plane, sign, row, column in ((0, 1, 0, 0), (1, -1, 0, 1), (1, 1, 1, 0), (0, 1, 1, 1)):
        high, low = high_low(prop[plane])
        if sign < 0:
            high, low = -high, -low
        rows = pl.ds(row * n, n)
        matrix[rows, pl.ds(column * n, n)] = high
        matrix[rows, pl.ds((2 + column) * n, n)] = low


def add_block(matrix, values, evolved, sums, ready=None):
    n = matrix.shape[0] // 2
    width = sums.shape[0]
    square, cross = sums.at[:, pl.ds(0, 2 * width)], sums.at[:, pl.ds(2 * width, width)]
    block = 256

    def evolve(index, carry):
        rows = pl.ds(pl.multiple_of(index * block, block), block)
        high = matrix[rows, pl.ds(0, 2 * n)]
        low = matrix[rows, pl.ds(2 * n, 2 * n)]
        evolved[rows, :] = (
            jnp.dot(high, values[pl.ds(0, 2 * n), :], preferred_element_type=jnp.float32)
            + jnp.dot(high, values[pl.ds(2 * n, 2 * n), :], preferred_element_type=jnp.float32)
            + jnp.dot(low, values[pl.ds(0, 2 * n), :], preferred_element_type=jnp.float32)
        )
        return carry

    lax.fori_loop(0, 2 * n // block, evolve, 0)
    if ready is not None:
        ready()
    high, low = high_low(evolved[...])
    both = jnp.concatenate([high, low], axis=1)
    turned_high = high.T
    turned_low = low[n:].T
    square[...] += jnp.dot(turned_high, both, preferred_element_type=jnp.float32)
    cross[...] += (
        jnp.dot(turned_high[:, n:], high[:n], preferred_element_type=jnp.float32)
        + jnp.dot(turned_high[:, n:], low[:n], preferred_element_type=jnp.float32)
        + jnp.dot(turned_low, high[:n], preferred_element_type=jnp.float32)
    )


def fill(values, n, plane, start, rows, block):
    high, low = high_low(block)
    values[pl.ds(plane * n + start, rows), :] = high
    values[pl.ds((2 + plane) * n + start, rows), :] = low


def density_early_body(count, prop, *refs):
    parts, (sums, matrix, values, evolved) = refs[:count], refs[count:]
    n = prop.shape[1]

    @pl.when(pl.program_id(0) == 0)
    def prepare():
        spread_propagator(prop, matrix)
        sums[...] = jnp.zeros_like(sums)

    me = lax.axis_index("cfg")
    for plane in range(2):
        for index, part in enumerate(parts):
            rows = part.shape[1]
            fill(values, n, plane, pl.multiple_of((me ^ index) * rows, rows), rows, part[plane])
    add_block(matrix, values, evolved, sums)


def density_late_body(matrix_far, parts, sums_far, keep, send, matrix, values, evolved, sums, sems):
    n = matrix.shape[0] // 2
    width = sums.shape[0]
    copies = [
        pltpu.make_async_copy(matrix_far, matrix, sems.at[0]),
        pltpu.make_async_copy(sums_far, sums, sems.at[1]),
    ]
    for copy in copies:
        copy.start()
    for plane in range(2):
        fill(values, n, plane, 0, n, parts[:, plane].reshape(n, width))
    copies[0].wait()

    add_block(matrix, values, evolved, sums, copies[1].wait)
    mixed = sums[:, width : 2 * width]
    cross = sums[:, 2 * width :]
    sums[:, :width] = sums[:, :width] + mixed + mixed.T
    sums[:, width : 2 * width] = cross - cross.T
    me = lax.axis_index("cfg")
    chip, core = jnp.right_shift(me, 1), me & 1
    inner, planes, own, _ = keep.shape
    for near in range(inner):
        for plane in range(planes):
            target = 2 * (chip ^ (plane * inner + near))
            mine = pl.ds(pl.multiple_of((target + core) * own, own), own)
            other = pl.ds(pl.multiple_of((target + 1 - core) * own, own), own)
            keep[near, plane] = sums[mine, pl.ds(0, 2 * width)]
            send[near, plane] = sums[other, pl.ds(0, 2 * width)]


def cost(slots, width, n):
    return pl.CostEstimate(flops=slots * width * n * (24 * n + 14 * width), bytes_accessed=2**24, transcendentals=0)


vmem = pl.BlockSpec(memory_space=pltpu.VMEM)
far = pl.BlockSpec(memory_space=pltpu.HBM)


def density_early(prop, parts, width):
    n = prop.shape[1]
    slots = parts[0].shape[-1] // width
    return pl.pallas_call(
        lambda *refs: density_early_body(len(parts), *refs),
        grid=(slots,),
        in_specs=[pl.BlockSpec((2, n, n), lambda i: (0, 0, 0)),
                  *(pl.BlockSpec((2, part.shape[1], width), lambda i: (0, 0, i)) for part in parts)],
        out_specs=(
            pl.BlockSpec((width, 3 * width), lambda i: (0, 0)),
            pl.BlockSpec((2 * n, 4 * n), lambda i: (0, 0)),
        ),
        out_shape=(
            jax.ShapeDtypeStruct((width, 3 * width), jnp.float32),
            jax.ShapeDtypeStruct((2 * n, 4 * n), jnp.bfloat16),
        ),
        scratch_shapes=[
            pltpu.VMEM((4 * n, width), jnp.bfloat16),
            pltpu.VMEM((2 * n, width), jnp.float32),
        ],
        compiler_params=pltpu.CompilerParams(dimension_semantics=("arbitrary",)),
        cost_estimate=cost(slots, width, n),
        name="density_early",
    )(prop, *parts)


def density_late(matrix, parts, sums, devices):
    n = matrix.shape[0] // 2
    width = sums.shape[0]
    half = jax.ShapeDtypeStruct((devices // 8, 4, width // devices, 2 * width), jnp.float32)
    return pl.pallas_call(
        density_late_body,
        in_specs=[far, vmem, far],
        out_specs=(vmem, vmem),
        out_shape=(half, half),
        scratch_shapes=[
            pltpu.VMEM(matrix.shape, jnp.bfloat16),
            pltpu.VMEM((4 * n, width), jnp.bfloat16),
            pltpu.VMEM((2 * n, width), jnp.float32),
            pltpu.VMEM((width, 3 * width), jnp.float32),
            pltpu.SemaphoreType.DMA((2,)),
        ],
        compiler_params=pltpu.CompilerParams(vmem_limit_bytes=48 * 2**20),
        cost_estimate=cost(1, width, n),
        name="density_late",
    )(matrix, parts, sums)


def exchange_order(devices):
    half = devices // 2
    return list(range(half, devices)) + list(range(1, half))


def shards(amplitudes, prop_third, first, second, third, steps, devices):
    width = amplitudes.shape[3]
    owned = amplitudes.shape[2] // devices
    late = 1
    members = devices // 4
    arrived = [None] * devices
    blocks = []
    for group in range(4):
        blocks += pack(amplitudes, first, second, third, steps, devices, 0, owned - late, group, members)
    arrived[0] = blocks[0]
    for distance in exchange_order(devices):
        pairs = [(i, i ^ distance) for i in range(devices)]
        arrived[distance] = lax.ppermute(blocks[distance], "cfg", pairs)
    packed = pack(amplitudes, first, second, third, steps, devices, owned - late, late, None, None)
    parts = lax.all_to_all(packed, "cfg", split_axis=0, concat_axis=0, tiled=True)
    sums, matrix = density_early(prop_third, arrived, width)
    keep, send = density_late(matrix, parts, sums, devices)
    return reduce_sums(keep, send, devices)


def passed(values, distance, devices):
    return lax.ppermute(values, "cfg", [(i, i ^ distance) for i in range(devices)])


def reduce_sums(keep, send, devices):
    inner, planes, own, lanes = keep.shape
    other = passed(send, 1, devices)
    near = [keep[k] + other[k] for k in range(inner)]
    arrived = [passed(near[k], 2 * k, devices) for k in range(inner - 1, 0, -1)]
    blocks = []
    for plane in range(planes):
        block = near[0][plane]
        for values in arrived:
            block = block + values[plane]
        blocks.append(block)
    total = blocks[0]
    for values in [passed(blocks[plane], 2 * inner * plane, devices) for plane in range(planes - 1, 0, -1)]:
        total = total + values
    return total.reshape(own, 2, lanes // 2)


def boundary_terms(first, second, third, detune_steps):
    scaled = detune_steps.astype(jnp.float32) * angle_step
    phase_first = scaled[0] * occupation(first)
    phase_second = scaled[1] * occupation(second)
    phase_third = scaled[2] * occupation(third)
    last_first = bit(first, 13)[None, None, :]
    near_first = bit(first, 12)[None, None, :]
    head_second = bit(second, 0)[None, :, None]
    next_second = bit(second, 1)[None, :, None]
    last_second = bit(second, 13)[None, :, None]
    near_second = bit(second, 12)[None, :, None]
    head_third = bit(third, 0)[:, None, None]
    next_third = bit(third, 1)[:, None, None]
    allowed = (1.0 - last_first * head_second) * (1.0 - last_second * head_third)
    pairs = (
        near_first * head_second
        + last_first * next_second
        + near_second * head_third
        + last_second * next_third
    )
    angle = (
        phase_third[:, None, None]
        + phase_second[None, :, None]
        + phase_first[None, None, :]
        + pair_angle * pairs
    )
    return (allowed, angle)


def apply_third(block, prop):

    def product(values, matrix):
        return jnp.einsum("ij,jba->iba", matrix, values, precision=lax.Precision.HIGHEST)

    real_part = product(block[0], prop[0]) - product(block[1], prop[1])
    imag_part = product(block[0], prop[1]) + product(block[1], prop[0])
    return jnp.stack([real_part, imag_part])


def inner_rows(left, right):
    return lax.dot_general(
        left,
        right,
        (((0,), (0,)), ((), ())),
        precision=lax.Precision.HIGHEST,
        preferred_element_type=jnp.float32,
    )


def plain_shards(amplitudes, prop_third, bitmasks_first, bitmasks_second, bitmasks_third, detune_steps):
    allowed, angle = boundary_terms(bitmasks_first, bitmasks_second, bitmasks_third, detune_steps)
    cosine = jnp.cos(angle)
    sine = jnp.sin(angle)
    phased = jnp.stack(
        [
            allowed * (amplitudes[0] * cosine + amplitudes[1] * sine),
            allowed * (amplitudes[1] * cosine - amplitudes[0] * sine),
        ]
    )
    evolved = apply_third(
        lax.all_to_all(phased, "cfg", split_axis=2, concat_axis=1, tiled=True), prop_third
    )
    width = evolved.shape[3]
    flat_real = evolved[0].reshape(-1, width)
    flat_imag = evolved[1].reshape(-1, width)
    stacked = jnp.concatenate([flat_real, flat_imag], axis=0)
    local_real = inner_rows(stacked, stacked)
    crossed = inner_rows(flat_imag, flat_real)
    local_term = jnp.stack([local_real, crossed - crossed.T], axis=1)
    return lax.psum_scatter(local_term, "cfg", scatter_dimension=0, tiled=True)


def solution(mesh):
    devices = mesh.shape["cfg"]

    def body(amplitudes, *others):
        rows = amplitudes.shape[1]
        seconds, width = amplitudes.shape[2:]
        powers = devices & (devices - 1) == 0
        if rows % 16 or devices % 8 or seconds != tile or seconds // devices < 2 or (width // devices) % 8 or width % tile or not powers:
            return plain_shards(amplitudes, *others)
        return shards(amplitudes, *others, devices)

    placed = (P("runs", "cfg", None, None), P(), P(), P(), P("cfg"), P("runs"))
    return jax.shard_map(
        body,
        mesh=mesh,
        in_specs=placed,
        out_specs=P(("runs", "cfg"), None, None),
        check_vma=False,
    )
```

```python
import jax
import jax.numpy as jnp
from jax import lax
from jax.experimental import pallas as pl
from jax.experimental.pallas import tpu as pltpu
from jax.sharding import PartitionSpec as P

angle_step = 0.2
pair_angle = 0.7
atom_count = 14
tile = 128
block = 512


def bit(masks, which):
    return (jnp.right_shift(masks, which) & 1).astype(jnp.float32)


def occupation(masks):
    total = bit(masks, 0)
    for which in range(1, atom_count):
        total = total + bit(masks, which)
    return total


def high_low(values):
    high = values.astype(jnp.bfloat16)
    low = (values - high.astype(jnp.float32)).astype(jnp.bfloat16)
    return high, low


def swapped_lanes(values, distance):
    lanes = values.shape[1]
    place = lax.broadcasted_iota(jnp.int32, values.shape, 1)
    up = pltpu.roll(values, lanes - distance, 1)
    down = pltpu.roll(values, distance, 1)
    return jnp.where((place & distance) == 0, up, down)


def phase_tables(shape, change, steps, third, first, second, tables):
    rows, seconds, owned, width, devices = shape
    row_re, row_im, col_re, col_im = tables
    scale_first = steps[0].astype(jnp.float32) * angle_step
    scale_second = steps[1].astype(jnp.float32) * angle_step
    scale_third = steps[2].astype(jnp.float32) * angle_step
    kind = lax.broadcasted_iota(jnp.int32, (8, width), 0)
    masks = jnp.broadcast_to(first[...], (8, width))
    head = bit(kind, 0)
    angle = scale_first * occupation(masks) + pair_angle * (
        bit(masks, 12) * head + bit(masks, 13) * bit(kind, 1)
    )
    allowed = 1.0 - bit(masks, 13) * head
    table_re = allowed * jnp.cos(angle)
    table_im = -allowed * jnp.sin(angle)
    for index in range(width // tile):
        row_re[pl.ds(8 * index, 8), :] = table_re[:, index * tile : (index + 1) * tile]
        row_im[pl.ds(8 * index, 8), :] = table_im[:, index * tile : (index + 1) * tile]
    place = lax.broadcasted_iota(jnp.int32, (rows, seconds), 0)
    masks_third = jnp.zeros((rows, seconds), jnp.int32)
    for row in range(rows):
        masks_third = jnp.where(place == row, third[row], masks_third)
    masks_second = jnp.broadcast_to(second[...], (rows, seconds))
    if change is not None:
        distance = 1
        while distance < devices:
            masks_second = jnp.where(
                (change & distance) != 0, swapped_lanes(masks_second, distance * owned), masks_second
            )
            distance *= 2
    last = bit(masks_second, 13)
    angle = (
        scale_third * occupation(masks_third)
        + scale_second * occupation(masks_second)
        + pair_angle * (bit(masks_second, 12) * bit(masks_third, 0) + last * bit(masks_third, 1))
    )
    allowed = 1.0 - last * bit(masks_third, 0)
    col_re[...] = allowed * jnp.cos(angle)
    col_im[...] = -allowed * jnp.sin(angle)


def phase_block(amps, out, tables, stride, state, kind, column, rows, width, lane):
    row_re, row_im, col_re, col_im = tables
    for half in range(0, rows, 8):
        down_re = col_re[pl.ds(half, 8), column : column + 1]
        down_im = col_im[pl.ds(half, 8), column : column + 1]
        for index in range(width // tile):
            across_re = row_re[pl.ds(8 * index + kind, 1), :]
            across_im = row_im[pl.ds(8 * index + kind, 1), :]
            turn_re = down_re * across_re - down_im * across_im
            turn_im = down_re * across_im + down_im * across_re
            real = amps[index][0, pl.ds(half * stride + state, 8, stride=stride), :]
            imag = amps[index][1, pl.ds(half * stride + state, 8, stride=stride), :]
            lanes = pl.ds(lane + index * tile, tile)
            out[0, pl.ds(half, 8), lanes] = real * turn_re - imag * turn_im
            out[1, pl.ds(half, 8), lanes] = real * turn_im + imag * turn_re


def pack_group_body(shape, slots, group, members, steps, third, second_smem, first, second, far, *refs):
    rows, _, owned, width, _ = shape
    packed, (amps, ready, *tables, arrivals, leaves) = refs[:members], refs[members:]
    tiles = width // tile
    stride = members * owned
    here = lax.axis_index("cfg")
    me = here & (members - 1)
    offset = (jnp.right_shift(here, members.bit_length() - 1) ^ group) * stride
    states = pl.ds(pl.multiple_of(offset, stride), stride)
    copies = [
        pltpu.make_async_copy(far.at[:, :, states, pl.ds(t * tile, tile)], amps.at[t], arrivals.at[t])
        for t in range(tiles)
    ]
    for copy in copies:
        copy.start()
    phase_tables(shape, here ^ (group * members), steps, third, first, second, tables)
    for copy in copies:
        copy.wait()
    flat = [amps.at[t].reshape(2, rows * stride, tile) for t in range(tiles)]
    sends = []
    for target in range(members):
        for slot in range(slots):
            state = (me ^ target) * owned + slot
            kind = second_smem[offset + state] & 3
            phase_block(flat, ready.at[target], tables, stride, state, kind, target * owned + slot, rows, width, slot * width)
        sends.append(pltpu.make_async_copy(ready.at[target], packed[target], leaves.at[target]))
        sends[-1].start()
    for send in sends:
        send.wait()


def pack_late_body(shape, slot, steps, third, second_smem, first, second, *refs):
    rows, seconds, owned, width, devices = shape
    tiles = width // tile
    flat = [ref.reshape(2, rows * seconds, tile) for ref in refs[:tiles]]
    packed, tables = refs[tiles], refs[tiles + 1 :]
    phase_tables(shape, None, steps, third, first, second, tables)
    for target in range(devices):
        state = target * owned + slot
        kind = second_smem[state] & 3
        phase_block(flat, packed.at[target], tables, seconds, state, kind, state, rows, width, 0)


def table_shapes(rows, seconds, width):
    return [pltpu.VMEM((8 * width // tile, tile), jnp.float32)] * 2 + [pltpu.VMEM((rows, seconds), jnp.float32)] * 2


smem = pl.BlockSpec(memory_space=pltpu.SMEM)
vmem = pl.BlockSpec(memory_space=pltpu.VMEM)
far = pl.BlockSpec(memory_space=pltpu.HBM)


def pack_cost(amps):
    return pl.CostEstimate(flops=6 * amps.size, bytes_accessed=2 * amps.size, transcendentals=0)


def pack_group(amps, first, second, third, steps, devices, slots, group, members):
    _, rows, seconds, width = amps.shape
    tiles = width // tile
    owned = seconds // devices
    shape = (rows, seconds, owned, width, devices)
    piece = (2, rows, slots * width)
    return pl.pallas_call(
        lambda *refs: pack_group_body(shape, slots, group, members, *refs),
        in_specs=[smem, smem, smem, vmem, vmem, far],
        out_specs=(far,) * members,
        out_shape=(jax.ShapeDtypeStruct(piece, jnp.float32),) * members,
        scratch_shapes=[
            pltpu.VMEM((tiles, 2, rows, members * owned, tile), jnp.float32),
            pltpu.VMEM((members, *piece), jnp.float32),
            *table_shapes(rows, seconds, width),
            pltpu.SemaphoreType.DMA((tiles,)),
            pltpu.SemaphoreType.DMA((members,)),
        ],
        cost_estimate=pack_cost(amps),
    )(steps, third, second, first.reshape(1, -1), second.reshape(1, -1), amps)


def pack_late(amps, first, second, third, steps, devices, slot):
    _, rows, seconds, width = amps.shape
    tiles = width // tile
    shape = (rows, seconds, seconds // devices, width, devices)
    whole = lambda n: pl.BlockSpec((1, n), lambda i: (0, 0))
    return pl.pallas_call(
        lambda *refs: pack_late_body(shape, slot, *refs),
        grid=(1,),
        in_specs=[smem, smem, smem, whole(width), whole(seconds),
                  *(pl.BlockSpec((2, rows, seconds, tile), lambda i, t=t: (0, 0, 0, t)) for t in range(tiles))],
        out_specs=pl.BlockSpec((devices, 2, rows, width), lambda i: (0, 0, 0, 0)),
        out_shape=jax.ShapeDtypeStruct((devices, 2, rows, width), jnp.float32),
        scratch_shapes=table_shapes(rows, seconds, width),
        cost_estimate=pack_cost(amps),
        name="pack_late",
    )(steps, third, second, first.reshape(1, -1), second.reshape(1, -1), *[amps] * tiles)


def spread_propagator(prop, matrix):
    n = prop.shape[1]
    for plane, sign, row, column in ((0, 1, 0, 0), (1, -1, 0, 1), (1, 1, 1, 0), (0, 1, 1, 1)):
        high, low = high_low(prop[plane])
        if sign < 0:
            high, low = -high, -low
        rows = pl.ds(row * n, n)
        matrix[rows, pl.ds(column * n, n)] = high
        matrix[rows, pl.ds((2 + column) * n, n)] = low


def add_block(matrix, values, evolved, sums, rows_ready=None, ready=None):
    n = matrix.shape[0] // 2
    width = sums.shape[0]
    square, cross = sums.at[:, pl.ds(0, 2 * width)], sums.at[:, pl.ds(2 * width, width)]

    def evolve(index, carry):
        rows = pl.ds(pl.multiple_of(index * block, block), block)
        if rows_ready is not None:
            rows_ready(rows, index)
        high = matrix[rows, pl.ds(0, 2 * n)]
        low = matrix[rows, pl.ds(2 * n, 2 * n)]
        evolved[rows, :] = (
            jnp.dot(high, values[pl.ds(0, 2 * n), :], preferred_element_type=jnp.float32)
            + jnp.dot(high, values[pl.ds(2 * n, 2 * n), :], preferred_element_type=jnp.float32)
            + jnp.dot(low, values[pl.ds(0, 2 * n), :], preferred_element_type=jnp.float32)
        )
        return carry

    lax.fori_loop(0, 2 * n // block, evolve, 0)
    if ready is not None:
        ready()
    high, low = high_low(evolved[...])
    both = jnp.concatenate([high, low], axis=1)
    turned_high = high.T
    turned_low = low[n:].T
    square[...] += jnp.dot(turned_high, both, preferred_element_type=jnp.float32)
    cross[...] += (
        jnp.dot(turned_high[:, n:], high[:n], preferred_element_type=jnp.float32)
        + jnp.dot(turned_high[:, n:], low[:n], preferred_element_type=jnp.float32)
        + jnp.dot(turned_low, high[:n], preferred_element_type=jnp.float32)
    )


def fill(values, n, plane, start, rows, block):
    high, low = high_low(block)
    values[pl.ds(plane * n + start, rows), :] = high
    values[pl.ds((2 + plane) * n + start, rows), :] = low


def density_early_body(count, prop, *refs):
    parts, (sums, matrix, values, evolved) = refs[:count], refs[count:]
    n = prop.shape[1]

    @pl.when(pl.program_id(0) == 0)
    def prepare():
        spread_propagator(prop, matrix)
        sums[...] = jnp.zeros_like(sums)

    me = lax.axis_index("cfg")
    for plane in range(2):
        for index, part in enumerate(parts):
            rows = part.shape[1]
            fill(values, n, plane, pl.multiple_of((me ^ index) * rows, rows), rows, part[plane])
    add_block(matrix, values, evolved, sums)


def density_late_body(matrix_far, parts, sums_far, keep, send, matrix, values, evolved, sums, sems):
    n = matrix.shape[0] // 2
    width = sums.shape[0]

    def matrix_copy(rows, index):
        return pltpu.make_async_copy(matrix_far.at[rows, :], matrix.at[rows, :], sems.at[index])

    pieces = 2 * n // block
    for index in range(pieces):
        matrix_copy(pl.ds(index * block, block), index).start()
    sums_copy = pltpu.make_async_copy(sums_far, sums, sems.at[pieces])
    sums_copy.start()
    for plane in range(2):
        fill(values, n, plane, 0, n, parts[:, plane].reshape(n, width))
    add_block(matrix, values, evolved, sums, lambda rows, index: matrix_copy(rows, index).wait(), sums_copy.wait)
    mixed = sums[:, width : 2 * width]
    cross = sums[:, 2 * width :]
    sums[:, :width] = sums[:, :width] + mixed + mixed.T
    sums[:, width : 2 * width] = cross - cross.T
    me = lax.axis_index("cfg")
    chip, core = jnp.right_shift(me, 1), me & 1
    inner, planes, own, _ = keep.shape
    for near in range(inner):
        for plane in range(planes):
            target = 2 * (chip ^ (plane * inner + near))
            mine = pl.ds(pl.multiple_of((target + core) * own, own), own)
            other = pl.ds(pl.multiple_of((target + 1 - core) * own, own), own)
            keep[near, plane] = sums[mine, pl.ds(0, 2 * width)]
            send[near, plane] = sums[other, pl.ds(0, 2 * width)]


def cost(slots, width, n):
    return pl.CostEstimate(flops=slots * width * n * (24 * n + 14 * width), bytes_accessed=2**24, transcendentals=0)


def density_early(prop, parts, width):
    n = prop.shape[1]
    slots = parts[0].shape[-1] // width
    return pl.pallas_call(
        lambda *refs: density_early_body(len(parts), *refs),
        grid=(slots,),
        in_specs=[pl.BlockSpec((2, n, n), lambda i: (0, 0, 0)),
                  *(pl.BlockSpec((2, part.shape[1], width), lambda i: (0, 0, i)) for part in parts)],
        out_specs=(
            pl.BlockSpec((width, 3 * width), lambda i: (0, 0)),
            pl.BlockSpec((2 * n, 4 * n), lambda i: (0, 0)),
        ),
        out_shape=(
            jax.ShapeDtypeStruct((width, 3 * width), jnp.float32),
            jax.ShapeDtypeStruct((2 * n, 4 * n), jnp.bfloat16),
        ),
        scratch_shapes=[
            pltpu.VMEM((4 * n, width), jnp.bfloat16),
            pltpu.VMEM((2 * n, width), jnp.float32),
        ],
        compiler_params=pltpu.CompilerParams(dimension_semantics=("arbitrary",)),
        cost_estimate=cost(slots, width, n),
        name="density_early",
    )(prop, *parts)


def density_late(matrix, parts, sums, devices):
    n = matrix.shape[0] // 2
    width = sums.shape[0]
    half = jax.ShapeDtypeStruct((devices // 8, 4, width // devices, 2 * width), jnp.float32)
    return pl.pallas_call(
        density_late_body,
        in_specs=[far, vmem, far],
        out_specs=(vmem, vmem),
        out_shape=(half, half),
        scratch_shapes=[
            pltpu.VMEM(matrix.shape, jnp.bfloat16),
            pltpu.VMEM((4 * n, width), jnp.bfloat16),
            pltpu.VMEM((2 * n, width), jnp.float32),
            pltpu.VMEM((width, 3 * width), jnp.float32),
            pltpu.SemaphoreType.DMA((2 * n // block + 1,)),
        ],
        compiler_params=pltpu.CompilerParams(vmem_limit_bytes=48 * 2**20),
        cost_estimate=cost(1, width, n),
        name="density_late",
    )(matrix, parts, sums)


def exchange_order(devices):
    half = devices // 2
    return list(range(half, devices)) + list(range(1, half))


def shards(amplitudes, prop_third, first, second, third, steps, devices):
    width = amplitudes.shape[3]
    owned = amplitudes.shape[2] // devices
    members = devices // 4
    arrived = [None] * devices
    blocks = []
    for group in range(4):
        blocks += pack_group(amplitudes, first, second, third, steps, devices, owned - 1, group, members)
    arrived[0] = blocks[0]
    for distance in exchange_order(devices):
        pairs = [(i, i ^ distance) for i in range(devices)]
        arrived[distance] = lax.ppermute(blocks[distance], "cfg", pairs)
    packed = pack_late(amplitudes, first, second, third, steps, devices, owned - 1)
    parts = lax.all_to_all(packed, "cfg", split_axis=0, concat_axis=0, tiled=True)
    sums, matrix = density_early(prop_third, arrived, width)
    keep, send = density_late(matrix, parts, sums, devices)
    return reduce_sums(keep, send, devices)


def passed(values, distance, devices):
    return lax.ppermute(values, "cfg", [(i, i ^ distance) for i in range(devices)])


def reduce_sums(keep, send, devices):
    inner, planes, own, lanes = keep.shape
    other = passed(send, 1, devices)
    near = [keep[k] + other[k] for k in range(inner)]
    arrived = [passed(near[k], 2 * k, devices) for k in range(inner - 1, 0, -1)]
    blocks = []
    for plane in range(planes):
        block = near[0][plane]
        for values in arrived:
            block = block + values[plane]
        blocks.append(block)
    total = blocks[0]
    for values in [passed(blocks[plane], 2 * inner * plane, devices) for plane in range(planes - 1, 0, -1)]:
        total = total + values
    return total.reshape(own, 2, lanes // 2)


def boundary_terms(first, second, third, detune_steps):
    scaled = detune_steps.astype(jnp.float32) * angle_step
    phase_first = scaled[0] * occupation(first)
    phase_second = scaled[1] * occupation(second)
    phase_third = scaled[2] * occupation(third)
    last_first = bit(first, 13)[None, None, :]
    near_first = bit(first, 12)[None, None, :]
    head_second = bit(second, 0)[None, :, None]
    next_second = bit(second, 1)[None, :, None]
    last_second = bit(second, 13)[None, :, None]
    near_second = bit(second, 12)[None, :, None]
    head_third = bit(third, 0)[:, None, None]
    next_third = bit(third, 1)[:, None, None]
    allowed = (1.0 - last_first * head_second) * (1.0 - last_second * head_third)
    pairs = (
        near_first * head_second
        + last_first * next_second
        + near_second * head_third
        + last_second * next_third
    )
    angle = (
        phase_third[:, None, None]
        + phase_second[None, :, None]
        + phase_first[None, None, :]
        + pair_angle * pairs
    )
    return (allowed, angle)


def apply_third(block, prop):

    def product(values, matrix):
        return jnp.einsum("ij,jba->iba", matrix, values, precision=lax.Precision.HIGHEST)

    real_part = product(block[0], prop[0]) - product(block[1], prop[1])
    imag_part = product(block[0], prop[1]) + product(block[1], prop[0])
    return jnp.stack([real_part, imag_part])


def inner_rows(left, right):
    return lax.dot_general(
        left,
        right,
        (((0,), (0,)), ((), ())),
        precision=lax.Precision.HIGHEST,
        preferred_element_type=jnp.float32,
    )


def plain_shards(amplitudes, prop_third, bitmasks_first, bitmasks_second, bitmasks_third, detune_steps):
    allowed, angle = boundary_terms(bitmasks_first, bitmasks_second, bitmasks_third, detune_steps)
    cosine = jnp.cos(angle)
    sine = jnp.sin(angle)
    phased = jnp.stack(
        [
            allowed * (amplitudes[0] * cosine + amplitudes[1] * sine),
            allowed * (amplitudes[1] * cosine - amplitudes[0] * sine),
        ]
    )
    evolved = apply_third(
        lax.all_to_all(phased, "cfg", split_axis=2, concat_axis=1, tiled=True), prop_third
    )
    width = evolved.shape[3]
    flat_real = evolved[0].reshape(-1, width)
    flat_imag = evolved[1].reshape(-1, width)
    stacked = jnp.concatenate([flat_real, flat_imag], axis=0)
    local_real = inner_rows(stacked, stacked)
    crossed = inner_rows(flat_imag, flat_real)
    local_term = jnp.stack([local_real, crossed - crossed.T], axis=1)
    return lax.psum_scatter(local_term, "cfg", scatter_dimension=0, tiled=True)


def solution(mesh):
    devices = mesh.shape["cfg"]

    def body(amplitudes, *others):
        rows = amplitudes.shape[1]
        seconds, width = amplitudes.shape[2:]
        powers = devices & (devices - 1) == 0
        if rows % 16 or devices % 8 or seconds != tile or seconds // devices < 2 or (width // devices) % 8 or width % tile or not powers:
            return plain_shards(amplitudes, *others)
        return shards(amplitudes, *others, devices)

    placed = (P("runs", "cfg", None, None), P(), P(), P(), P("cfg"), P("runs"))
    return jax.shard_map(
        body,
        mesh=mesh,
        in_specs=placed,
        out_specs=P(("runs", "cfg"), None, None),
        check_vma=False,
    )
```
